32 devices in a mesh: ka: 2 (over x), band: 16 (over z, y, core).
Axes of the slice: x: 2, y: 2, z: 4, core: 2. Of those that a mesh axis runs over, the one named last changes fastest.
Arguments:
- psi_hat: float32 [2, 12, 2, 128, 128, 128], P('ka', None, None, 'band'), may hold values from -1.5 to 1.5
- occupations: int32 [2, 12], P('ka'), may hold values from 0 to 2
- weights: int32 [2], P('ka'), may hold values from 1 to 6
- density_in: float32 [128, 128, 128], P('band'), may hold values from -12 to 12
- dens_hist: float32 [8, 128, 128, 128], P(None, 'band'), may hold values from -3 to 3
- resid_hist: float32 [8, 128, 128, 128], P(None, 'band'), may hold values from -12 to 12
Outputs:
- out_density: float32 [128, 128, 128], P('band')
- mixed_density: float32 [128, 128, 128], P('band')
The draws below stay inside these ranges and needn't reach their ends.
All inputs are finite; a program needn't handle non-finite values.
Results may differ from the reference program's by a relative error of at most 0.0003.
Values sent between devices are 32-bit elements; how exact they have to be, the bound alone decides.
No kernel may reach another device: no remote copies, remote signals or barrier semaphores. Data moves between devices by JAX's collectives and lax.ppermute only.
A program may use at most 128 MiB of HBM per device.

```python
from functools import partial
import jax
import jax.numpy as jnp
from jax import lax

NG = 128
BANDS = 12
HIST = 8
KPTS = 2


def common_field(key):
    return jax.random.truncated_normal(jax.random.fold_in(key, 7), -5.0, 5.0, (NG, NG, NG), jnp.float32)


def draw_density_in(key, part):
    shared = common_field(key)
    noise_part = jax.random.truncated_normal(jax.random.fold_in(key, 11), -5.0, 5.0, (NG, NG, NG), jnp.float32)
    return shared + 0.3 * noise_part


def draw_resid_hist(key, part):
    shared = common_field(key)
    loadings = jax.random.uniform(jax.random.fold_in(key, 13), (HIST, 1, 1, 1), jnp.float32, -1.0, 1.0)
    noise_part = jax.random.truncated_normal(jax.random.fold_in(key, 17), -5.0, 5.0, (HIST, NG, NG, NG), jnp.float32)
    return loadings * shared + 0.5 * noise_part


def touch_ends(array, stream_key, least, largest):
    longest = array.shape.index(max(array.shape))
    spots = []
    for shift in (0, 1):
        where = [jax.random.randint(jax.random.fold_in(stream_key, axis), (), 0, length) for axis, length in enumerate(array.shape)]
        where[longest] = (where[longest] + shift) % array.shape[longest]
        spots.append(tuple(where))
    return array.at[spots[0]].set(least).at[spots[1]].set(largest)


def level_of(stream_key, dims, split, smallest, top_value):
    level = 1.0
    for dim, parts in split:
        heights = jax.random.uniform(jax.random.fold_in(jax.random.fold_in(stream_key, 6), dim), (parts,), jnp.float32, smallest / len(split), top_value / len(split))
        level = level * jnp.repeat(jnp.exp(heights), dims[dim] // parts).reshape((-1,) + (1,) * (len(dims) - 1 - dim))
    return level


def gaussian(stream_key, shape, deviation, most, cuts=(), kind=jnp.bfloat16):
    gain = level_of(stream_key, shape, cuts, -0.22, 0.18) if cuts else 1.0
    result = jax.random.normal(stream_key, shape, jnp.float32) * deviation * gain
    return jnp.minimum(jnp.maximum(result, -most), most).astype(kind)


def setup_inputs(seed: int = 0) -> dict:
    key_list = jax.random.split(jax.random.key(seed), 7)
    psi_hat = gaussian(key_list[0], (KPTS, BANDS, 2, NG, NG, NG), 0.25, 1.5, ((0, 2), (3, 16)), jnp.float32)
    occupations = touch_ends(jax.random.randint(key_list[1], (KPTS, BANDS), 0, 3), jax.random.fold_in(key_list[1], 1), 0, 2).astype(jnp.int32)
    weights = jax.random.randint(key_list[2], (KPTS,), 1, 7).astype(jnp.int32)
    density_in = draw_density_in(jax.random.fold_in(key_list[6], 71), 0)
    dens_hist = gaussian(key_list[4], (HIST, NG, NG, NG), 0.5, 3.0, ((1, 16),), jnp.float32)
    resid_hist = draw_resid_hist(jax.random.fold_in(key_list[6], 71), 0)
    return dict(psi_hat=psi_hat, occupations=occupations, weights=weights, density_in=density_in, dens_hist=dens_hist, resid_hist=resid_hist)


highest = lax.Precision.HIGHEST
beta_mix = 0.3
regular = 0.01

def dft_tables():
    indices = jnp.arange(NG, dtype=jnp.int32)
    product = indices[:, None] * indices[None, :] % NG
    angles = product.astype(jnp.float32) * jnp.float32(2.0 * 3.141592653589793 / NG)
    return (jnp.cos(angles), jnp.sin(angles))

def rotate(pattern, real_part, imag_part, cosine_table, sine_table):
    einsum = partial(jnp.einsum, precision=highest)
    out_real = einsum(pattern, real_part, cosine_table) - einsum(pattern, imag_part, sine_table)
    out_imag = einsum(pattern, real_part, sine_table) + einsum(pattern, imag_part, cosine_table)
    return (out_real, out_imag)

def band_power(coeffs, cosine_table, sine_table):
    real_part, imag_part = rotate('pqk,kz->zpq', coeffs[0], coeffs[1], cosine_table, sine_table)
    real_part, imag_part = rotate('zpq,qy->zpy', real_part, imag_part, cosine_table, sine_table)
    real_part, imag_part = rotate('zpy,px->zxy', real_part, imag_part, cosine_table, sine_table)
    return (real_part * real_part + imag_part * imag_part) * jnp.float32(1.0 / NG ** 3)

def broyden(density, density_in, dens_hist, resid_hist):
    residual_now = density - density_in
    gram = jnp.einsum('hzxy,gzxy->hg', resid_hist, resid_hist, precision=highest)
    projections = jnp.einsum('hzxy,zxy->h', resid_hist, residual_now, precision=highest)
    system = gram + regular * jnp.diag(jnp.diag(gram))
    chol_factor = jnp.linalg.cholesky(system)
    mix_coefs = jax.scipy.linalg.cho_solve((chol_factor, True), projections)
    update = jnp.einsum('h,hzxy->zxy', mix_coefs, dens_hist + beta_mix * resid_hist, precision=highest)
    return density_in + beta_mix * residual_now - update

def reference(psi_hat, occupations, weights, density_in, dens_hist, resid_hist):
    cosine_table, sine_table = dft_tables()
    weight_total = jnp.sum(weights.astype(jnp.float32))

    def per_point(point_total, point_inputs):
        coeffs_point, occ_point, weight_point = point_inputs

        def per_band(band_total, band_inputs):
            coeffs_band, occ_band = band_inputs
            power = band_power(coeffs_band, cosine_table, sine_table)
            return (band_total + occ_band.astype(jnp.float32) * power, None)
        pool_term, unused = lax.scan(per_band, jnp.zeros((NG, NG, NG), jnp.float32), (coeffs_point, occ_point))
        return (point_total + pool_term * (weight_point.astype(jnp.float32) / weight_total), None)
    density, unused = lax.scan(per_point, jnp.zeros((NG, NG, NG), jnp.float32), (psi_hat, occupations, weights))
    mixed_density = broyden(density, density_in, dens_hist, resid_hist)
    return (density, mixed_density)
```

```python
import jax
import jax.numpy as jnp
import ml_dtypes
import numpy as np
from functools import partial
from jax import lax
from jax.experimental import pallas as pl
from jax.experimental.pallas import tpu as pltpu
from jax.sharding import PartitionSpec as P

highest = lax.Precision.HIGHEST
beta_mix = 0.3
regular = 0.01
bf16 = jnp.bfloat16


def tables(ng):
    idx = np.arange(ng, dtype=np.int64)
    angle = (idx[:, None] * idx[None, :] % ng) * (2.0 * np.pi / ng)
    cos, sin = np.cos(angle), np.sin(angle)
    full = np.block([[cos, sin], [-sin, cos]]).astype(np.float32)
    high = full.astype(ml_dtypes.bfloat16)
    low = (full - high.astype(np.float32)).astype(ml_dtypes.bfloat16)
    right = np.concatenate([high, high, low], axis=0)
    return np.ascontiguousarray(right.T), right


def split(value, axis):
    high = value.astype(bf16)
    low = (value - high.astype(jnp.float32)).astype(bf16)
    return jnp.concatenate([high, low, high], axis=axis)


def pre_kernel(psi_ref, left_ref, right_ref, out_ref, *, ng, planes, devs):
    depth = ng // devs
    left, right = left_ref[...], right_ref[...]
    for p0 in range(0, planes, 2):
        group = range(p0, min(p0 + 2, planes))
        rows = [
            jnp.concatenate([psi_ref[0, 0, 0, p], psi_ref[0, 0, 1, p]], axis=1) for p in group
        ]
        data = split(jnp.concatenate(rows, axis=0), 1)
        along_z = lax.dot_general(
            left, data, (((1,), (1,)), ((), ())), preferred_element_type=jnp.float32
        )
        for k, p in enumerate(group):
            cols = slice(k * ng, (k + 1) * ng)
            mid = jnp.concatenate([along_z[:ng, cols], along_z[ng:, cols]], axis=1)
            done = jnp.dot(split(mid, 1), right, preferred_element_type=jnp.float32)
            for part in range(2):
                piece = done[:, part * ng : (part + 1) * ng].reshape(devs, depth, ng)
                out_ref[:, 0, part, p * depth : (p + 1) * depth, :] = piece


def pre(psi_hat, left, right, first, count, devs):
    _, _, _, planes, ng, _ = psi_hat.shape
    depth = ng // devs
    return pl.pallas_call(
        partial(pre_kernel, ng=ng, planes=planes, devs=devs),
        grid=(count,),
        in_specs=[
            pl.BlockSpec((1, 1, 2, planes, ng, ng), lambda b: (0, first + b, 0, 0, 0, 0)),
            pl.BlockSpec(left.shape, lambda b: (0, 0)),
            pl.BlockSpec(right.shape, lambda b: (0, 0)),
        ],
        out_specs=pl.BlockSpec((devs, 1, 2, planes * depth, ng), lambda b: (0, b, 0, 0, 0)),
        out_shape=jax.ShapeDtypeStruct((devs, count, 2, planes * depth, ng), jnp.float32),
        name="pre",
    )(psi_hat, left, right)


def post_kernel(scale_ref, recv_ref, left_ref, *rest, ng, planes, devs, first, fresh, last):
    rest = list(rest)
    prev_ref = None if fresh else rest.pop(0)
    resid_ref = rest.pop(0) if last else None
    pool_ref = rest[0]
    depth = ng // devs
    band = pl.program_id(0)

    @pl.when(band == 0)
    def _():
        pool_ref[...] = jnp.zeros_like(pool_ref) if fresh else prev_ref[...]

    left = left_ref[...]
    scale = scale_ref[first + band]
    for j0 in range(0, depth, 2):
        group = range(j0, min(j0 + 2, depth))
        cols = []
        for j in group:
            pieces = [
                recv_ref[d, 0, part, pl.ds(j, planes, stride=depth), :]
                for part in range(2)
                for d in range(devs)
            ]
            cols.append(jnp.concatenate(pieces, axis=0))
        data = split(jnp.concatenate(cols, axis=1), 0)
        field = jnp.dot(left, data, preferred_element_type=jnp.float32)
        power = (field[:ng] * field[:ng] + field[ng:] * field[ng:]) * scale
        for k, j in enumerate(group):
            pool_ref[j] += power[:, k * ng : (k + 1) * ng]

    if last:
        proj_ref = rest[1]

        @pl.when(band == pl.num_programs(0) - 1)
        def _():
            for h in range(resid_ref.shape[0]):
                total = jnp.zeros((8, ng), jnp.float32)
                for j in range(depth):
                    term = resid_ref[h, j] * pool_ref[j]
                    total = total + jnp.sum(term.reshape(ng // 8, 8, ng), axis=0)
                proj_ref[h : h + 1, :] = jnp.sum(total, axis=0, keepdims=True)


def post(scales, recv, left, prev, resid, first):
    devs, count, _, cells, ng = recv.shape
    depth = ng // devs
    planes = cells // depth
    slab = pl.BlockSpec((depth, ng, ng), lambda b: (0, 0, 0))
    args = [scales, recv, left]
    in_specs = [
        pl.BlockSpec(memory_space=pltpu.SMEM),
        pl.BlockSpec((devs, 1, 2, cells, ng), lambda b: (0, b, 0, 0, 0)),
        pl.BlockSpec(left.shape, lambda b: (0, 0)),
    ]
    out_specs = [slab]
    out_shape = [jax.ShapeDtypeStruct((depth, ng, ng), jnp.float32)]
    if prev is not None:
        args.append(prev)
        in_specs.append(slab)
    if resid is not None:
        hist = resid.shape[0]
        args.append(resid)
        in_specs.append(pl.BlockSpec(resid.shape, lambda b: (0, 0, 0, 0)))
        out_specs.append(pl.BlockSpec((hist, ng), lambda b: (0, 0)))
        out_shape.append(jax.ShapeDtypeStruct((hist, ng), jnp.float32))
    return pl.pallas_call(
        partial(
            post_kernel,
            ng=ng,
            planes=planes,
            devs=devs,
            first=first,
            fresh=prev is None,
            last=resid is not None,
        ),
        grid=(count,),
        in_specs=in_specs,
        out_specs=out_specs,
        out_shape=out_shape,
        name="post",
    )(*args)


def mix_kernel(inverse_ref, base_dot_ref, proj_ref, mine_ref, other_ref, base_ref, dir_ref,
               density_ref, mixed_ref):
    hist = dir_ref.shape[0]
    projections = jnp.sum(proj_ref[...], axis=1, keepdims=True) - base_dot_ref[...]
    coefs = jnp.sum(inverse_ref[...] * projections, axis=0, keepdims=True)
    density = mine_ref[0] + other_ref[0]
    base = base_ref[0]
    mixed = base + beta_mix * (density - base)
    for h in range(hist):
        mixed = mixed - coefs[:, h : h + 1] * dir_ref[h, 0]
    density_ref[0] = density
    mixed_ref[0] = mixed


def mix(inverse, base_dot, proj, mine, other, base, directions):
    depth, ng, _ = base.shape
    hist = directions.shape[0]
    slab = pl.BlockSpec((1, ng, ng), lambda j: (j, 0, 0))
    whole = lambda shape: pl.BlockSpec(shape, lambda j: (0, 0))
    return pl.pallas_call(
        mix_kernel,
        grid=(depth,),
        in_specs=[
            whole(inverse.shape),
            whole(base_dot.shape),
            whole(proj.shape),
            slab,
            slab,
            slab,
            pl.BlockSpec((hist, 1, ng, ng), lambda j: (0, j, 0, 0)),
        ],
        out_specs=[slab, slab],
        out_shape=[jax.ShapeDtypeStruct(base.shape, jnp.float32)] * 2,
        name="mix",
    )(inverse, base_dot, proj, mine, other, base, directions)


def tree_sum(value, axes_sizes):
    for axis, size in axes_sizes:
        if size & (size - 1):
            value = jnp.sum(lax.all_gather(value, axis), axis=0)
            continue
        step = 1
        while step < size:
            value = value + lax.ppermute(value, axis, [(i, i ^ step) for i in range(size)])
            step *= 2
    return value


def chunks_of(bands):
    edge = max(1, bands // 6)
    if bands <= 2 * edge:
        return [(0, bands)]
    return [(0, edge), (edge, bands - 2 * edge), (bands - edge, edge)]


def shards(psi_hat, occupations, weights, density_in, dens_hist, resid_hist, *, ka, devs):
    bands, ng = psi_hat.shape[1], psi_hat.shape[-1]
    left, right = (jnp.asarray(t) for t in tables(ng))
    chunks = chunks_of(bands)
    received = []
    for first, count in chunks:
        sent = pre(psi_hat, left, right, first, count, devs)
        received.append(lax.all_to_all(sent, "band", 0, 0, tiled=True))

    weight_total = lax.psum(jnp.sum(weights.astype(jnp.float32)), "ka")
    share = weights[0].astype(jnp.float32) / weight_total
    scales = occupations[0].astype(jnp.float32) * share * jnp.float32(1.0 / ng**3)

    einsum = partial(jnp.einsum, precision=highest)
    gram = einsum("hzxy,gzxy->hg", resid_hist, resid_hist)
    base_dot = einsum("hzxy,zxy->h", resid_hist, density_in)[:, None]
    gathered = lax.all_gather(jnp.concatenate([gram, base_dot], axis=1), "band")
    summed = jnp.sum(gathered, axis=0)
    gram, base_dot = summed[:, :-1], summed[:, -1:]
    system = gram + regular * jnp.diag(jnp.diag(gram))
    factor = jnp.linalg.cholesky(system)
    inverse = jax.scipy.linalg.cho_solve((factor, True), jnp.eye(gram.shape[0], dtype=jnp.float32))
    directions = dens_hist + beta_mix * resid_hist

    pool = None
    for (first, count), recv in zip(chunks, received):
        last = first + count == bands
        outs = post(scales, recv, left, pool, resid_hist if last else None, first)
        pool = outs[0]
    proj = outs[1]
    if ka == 2:
        mine, other = pool, lax.ppermute(pool, "ka", [(0, 1), (1, 0)])
    else:
        mine, other = lax.psum(pool, "ka"), jnp.zeros_like(pool)
    proj = tree_sum(proj, (("band", devs), ("ka", ka)))
    density, mixed = mix(inverse, base_dot, proj, mine, other, density_in, directions)
    return density, mixed


def solution(mesh):
    return jax.shard_map(
        partial(shards, ka=mesh.shape["ka"], devs=mesh.shape["band"]),
        mesh=mesh,
        in_specs=(
            P("ka", None, None, "band", None, None),
            P("ka", None),
            P("ka"),
            P("band", None, None),
            P(None, "band", None, None),
            P(None, "band", None, None),
        ),
        out_specs=(P("band", None, None), P("band", None, None)),
        check_vma=False,
    )
```

```python
import jax
import jax.numpy as jnp
import ml_dtypes
import numpy as np
from functools import partial
from jax import lax
from jax.experimental import pallas as pl
from jax.experimental.pallas import tpu as pltpu
from jax.sharding import PartitionSpec as P

highest = lax.Precision.HIGHEST
beta_mix = 0.3
regular = 0.01
bf16 = jnp.bfloat16


def tables(ng):
    idx = np.arange(ng, dtype=np.int64)
    angle = (idx[:, None] * idx[None, :] % ng) * (2.0 * np.pi / ng)
    cos, sin = np.cos(angle), np.sin(angle)
    full = np.block([[cos, sin], [-sin, cos]]).astype(np.float32)
    high = full.astype(ml_dtypes.bfloat16)
    low = (full - high.astype(np.float32)).astype(ml_dtypes.bfloat16)
    right = np.concatenate([high, high, low], axis=0)
    return np.ascontiguousarray(right.T), right


def split(value, axis):
    high = value.astype(bf16)
    low = (value - high.astype(jnp.float32)).astype(bf16)
    return jnp.concatenate([high, low, high], axis=axis)


def pre_kernel(psi_ref, left_ref, right_ref, out_ref, *, ng, planes, devs):
    depth = ng // devs
    left, right = left_ref[...], right_ref[...]
    for p0 in range(0, planes, 2):
        group = range(p0, min(p0 + 2, planes))
        rows = [
            jnp.concatenate([psi_ref[0, 0, 0, p], psi_ref[0, 0, 1, p]], axis=1) for p in group
        ]
        data = split(jnp.concatenate(rows, axis=0), 1)
        along_z = lax.dot_general(
            left, data, (((1,), (1,)), ((), ())), preferred_element_type=jnp.float32
        )
        for k, p in enumerate(group):
            cols = slice(k * ng, (k + 1) * ng)
            mid = jnp.concatenate([along_z[:ng, cols], along_z[ng:, cols]], axis=1)
            done = jnp.dot(split(mid, 1), right, preferred_element_type=jnp.float32)
            for part in range(2):
                piece = done[:, part * ng : (part + 1) * ng].reshape(devs, depth, ng)
                out_ref[:, 0, part, p * depth : (p + 1) * depth, :] = piece


def pre(psi_hat, left, right, first, count, devs):
    _, _, _, planes, ng, _ = psi_hat.shape
    depth = ng // devs
    return pl.pallas_call(
        partial(pre_kernel, ng=ng, planes=planes, devs=devs),
        grid=(count,),
        in_specs=[
            pl.BlockSpec((1, 1, 2, planes, ng, ng), lambda b: (0, first + b, 0, 0, 0, 0)),
            pl.BlockSpec(left.shape, lambda b: (0, 0)),
            pl.BlockSpec(right.shape, lambda b: (0, 0)),
        ],
        out_specs=pl.BlockSpec((devs, 1, 2, planes * depth, ng), lambda b: (0, b, 0, 0, 0)),
        out_shape=jax.ShapeDtypeStruct((devs, count, 2, planes * depth, ng), jnp.float32),
        name="pre",
    )(psi_hat, left, right)


def post_kernel(scale_ref, recv_ref, left_ref, *rest, ng, planes, devs, first, fresh, last):
    rest = list(rest)
    prev_ref = None if fresh else rest.pop(0)
    resid_ref = rest.pop(0) if last else None
    pool_ref = rest[0]
    depth = ng // devs
    band = pl.program_id(0)

    @pl.when(band == 0)
    def _():
        pool_ref[...] = jnp.zeros_like(pool_ref) if fresh else prev_ref[...]

    left = left_ref[...]
    scale = scale_ref[first + band]
    for j0 in range(0, depth, 2):
        group = range(j0, min(j0 + 2, depth))
        cols = []
        for j in group:
            pieces = [
                recv_ref[d, 0, part, pl.ds(j, planes, stride=depth), :]
                for part in range(2)
                for d in range(devs)
            ]
            cols.append(jnp.concatenate(pieces, axis=0))
        data = split(jnp.concatenate(cols, axis=1), 0)
        field = jnp.dot(left, data, preferred_element_type=jnp.float32)
        power = (field[:ng] * field[:ng] + field[ng:] * field[ng:]) * scale
        for k, j in enumerate(group):
            pool_ref[j] += power[:, k * ng : (k + 1) * ng]

    if last:
        proj_ref = rest[1]

        @pl.when(band == pl.num_programs(0) - 1)
        def _():
            for h in range(resid_ref.shape[0]):
                total = jnp.zeros((8, ng), jnp.float32)
                for j in range(depth):
                    term = resid_ref[h, j] * pool_ref[j]
                    total = total + jnp.sum(term.reshape(ng // 8, 8, ng), axis=0)
                proj_ref[h : h + 1, :] = jnp.sum(total, axis=0, keepdims=True)


def post(scales, recv, left, prev, resid, first):
    devs, count, _, cells, ng = recv.shape
    depth = ng // devs
    planes = cells // depth
    slab = pl.BlockSpec((depth, ng, ng), lambda b: (0, 0, 0))
    args = [scales, recv, left]
    in_specs = [
        pl.BlockSpec(memory_space=pltpu.SMEM),
        pl.BlockSpec((devs, 1, 2, cells, ng), lambda b: (0, b, 0, 0, 0)),
        pl.BlockSpec(left.shape, lambda b: (0, 0)),
    ]
    out_specs = [slab]
    out_shape = [jax.ShapeDtypeStruct((depth, ng, ng), jnp.float32)]
    if prev is not None:
        args.append(prev)
        in_specs.append(slab)
    if resid is not None:
        hist = resid.shape[0]
        args.append(resid)
        in_specs.append(pl.BlockSpec(resid.shape, lambda b: (0, 0, 0, 0)))
        out_specs.append(pl.BlockSpec((hist, ng), lambda b: (0, 0)))
        out_shape.append(jax.ShapeDtypeStruct((hist, ng), jnp.float32))
    return pl.pallas_call(
        partial(
            post_kernel,
            ng=ng,
            planes=planes,
            devs=devs,
            first=first,
            fresh=prev is None,
            last=resid is not None,
        ),
        grid=(count,),
        in_specs=in_specs,
        out_specs=out_specs,
        out_shape=out_shape,
        name="post",
    )(*args)


def mix_kernel(inverse_ref, base_dot_ref, proj_ref, mine_ref, other_ref, base_ref, dir_ref,
               density_ref, mixed_ref):
    hist = dir_ref.shape[0]
    projections = jnp.sum(proj_ref[...], axis=1, keepdims=True) - base_dot_ref[...]
    coefs = jnp.sum(inverse_ref[...] * projections, axis=0, keepdims=True)
    density = mine_ref[0] + other_ref[0]
    base = base_ref[0]
    mixed = base + beta_mix * (density - base)
    for h in range(hist):
        mixed = mixed - coefs[:, h : h + 1] * dir_ref[h, 0]
    density_ref[0] = density
    mixed_ref[0] = mixed


def mix(inverse, base_dot, proj, mine, other, base, directions):
    depth, ng, _ = base.shape
    hist = directions.shape[0]
    slab = pl.BlockSpec((1, ng, ng), lambda j: (j, 0, 0))
    whole = lambda shape: pl.BlockSpec(shape, lambda j: (0, 0))
    return pl.pallas_call(
        mix_kernel,
        grid=(depth,),
        in_specs=[
            whole(inverse.shape),
            whole(base_dot.shape),
            whole(proj.shape),
            slab,
            slab,
            slab,
            pl.BlockSpec((hist, 1, ng, ng), lambda j: (0, j, 0, 0)),
        ],
        out_specs=[slab, slab],
        out_shape=[jax.ShapeDtypeStruct(base.shape, jnp.float32)] * 2,
        name="mix",
    )(inverse, base_dot, proj, mine, other, base, directions)


def tree_sum(value, axes_sizes):
    for axis, size in axes_sizes:
        if size & (size - 1):
            value = jnp.sum(lax.all_gather(value, axis), axis=0)
            continue
        step = 1
        while step < size:
            value = value + lax.ppermute(value, axis, [(i, i ^ step) for i in range(size)])
            step *= 2
    return value


def chunks_of(bands):
    edge = max(1, bands // 12)
    if bands <= 2 * edge:
        return [(0, bands)]
    return [(0, edge), (edge, bands - 2 * edge), (bands - edge, edge)]


def history(resid_hist, dens_hist, density_in):
    einsum = partial(jnp.einsum, precision=highest)
    gram = einsum("hzxy,gzxy->hg", resid_hist, resid_hist)
    base_dot = einsum("hzxy,zxy->h", resid_hist, density_in)[:, None]
    gathered = lax.all_gather(jnp.concatenate([gram, base_dot], axis=1), "band")
    summed = jnp.sum(gathered, axis=0)
    gram, base_dot = summed[:, :-1], summed[:, -1:]
    system = gram + regular * jnp.diag(jnp.diag(gram))
    factor = jnp.linalg.cholesky(system)
    inverse = jax.scipy.linalg.cho_solve((factor, True), jnp.eye(gram.shape[0], dtype=jnp.float32))
    return inverse, base_dot, dens_hist + beta_mix * resid_hist


def shards(psi_hat, occupations, weights, density_in, dens_hist, resid_hist, *, ka, devs):
    bands, ng = psi_hat.shape[1], psi_hat.shape[-1]
    left, right = (jnp.asarray(t) for t in tables(ng))
    weight_total = lax.psum(jnp.sum(weights.astype(jnp.float32)), "ka")
    share = weights[0].astype(jnp.float32) / weight_total
    scales = occupations[0].astype(jnp.float32) * share * jnp.float32(1.0 / ng**3)

    chunks = chunks_of(bands)
    sent = [pre(psi_hat, left, right, first, count, devs) for first, count in chunks]
    exchange = lambda value: lax.all_to_all(value, "band", 0, 0, tiled=True)
    received = exchange(sent[0])
    received, resid_late, dens_late = lax.optimization_barrier((received, resid_hist, dens_hist))
    inverse, base_dot, directions = history(resid_late, dens_late, density_in)
    pool = None
    for step, (first, count) in enumerate(chunks):
        last = step == len(chunks) - 1
        outs = post(scales, received, left, pool, resid_hist if last else None, first)
        pool = outs[0]
        if last:
            break
        following = exchange(sent[1]) if step == 0 else pending
        if step + 2 < len(chunks):
            late, pool, inverse, base_dot, directions = lax.optimization_barrier(
                (sent[step + 2], pool, inverse, base_dot, directions)
            )
            pending = exchange(late)
        received = following
    proj = outs[1]
    if ka == 2:
        mine, other = pool, lax.ppermute(pool, "ka", [(0, 1), (1, 0)])
    else:
        mine, other = lax.psum(pool, "ka"), jnp.zeros_like(pool)
    proj = tree_sum(proj, (("band", devs), ("ka", ka)))
    density, mixed = mix(inverse, base_dot, proj, mine, other, density_in, directions)
    return density, mixed


def solution(mesh):
    return jax.shard_map(
        partial(shards, ka=mesh.shape["ka"], devs=mesh.shape["band"]),
        mesh=mesh,
        in_specs=(
            P("ka", None, None, "band", None, None),
            P("ka", None),
            P("ka"),
            P("band", None, None),
            P(None, "band", None, None),
            P(None, "band", None, None),
        ),
        out_specs=(P("band", None, None), P("band", None, None)),
        check_vma=False,
    )
```
